128 devices in a mesh: slab: 32 (over z, y, core), sub: 4 (over x).
Axes of the slice: x: 4, y: 4, z: 4, core: 2. Of those that a mesh axis runs over, the one named last changes fastest.
Arguments:
- factor_obs: float32 [128, 64, 64, 512], P('slab', 'sub'), may hold values from -0.1484375 to 0.1484375
- factor_ctrl: float32 [128, 64, 64, 512], P('slab', 'sub'), may hold values from -0.1484375 to 0.1484375
- diffusivity: float32 [128, 4096], P('slab', 'sub'), may hold values from 0.5 to 2
- input_map: float32 [4, 128, 4096], P(None, 'slab', 'sub'), may hold values from -1 to 1
- output_map: float32 [4, 128, 4096], P(None, 'slab', 'sub'), may hold values from -1 to 1
- start_block: float32 [512, 128], replicated, may hold values from -6 to 6
- order: int32 [1], replicated, may hold values from 64 to 128
Outputs:
- reduced_mass: float32 [128, 128], replicated
- reduced_state: float32 [128, 128], replicated
- reduced_input: float32 [128, 4], replicated
- reduced_output: float32 [4, 128], replicated
The draws below stay inside these ranges and needn't reach their ends.
All inputs are finite; a program needn't handle non-finite values.
Results may differ from the reference program's by a relative error of at most 0.00017.
Values sent between devices are 32-bit elements; how exact they have to be, the bound alone decides.
A program may use at most 128 MiB of HBM per device.

```python
import math
import jax
import jax.numpy as jnp
from jax import lax

NX = 64
RANK = 512
RMAX = 128
NIN = 4
NOUT = 4
POWER = 2
NZ = 128
NY = 64
NYX = 4096
NCELL = 524288


def factor_draw(key, salt):
    key = jax.random.fold_in(key, salt)
    entry_key, level_key = jax.random.split(key)
    entries = jnp.clip(jax.random.normal(entry_key, (NZ, NY, NX, RANK), jnp.float32), -6.0, 6.0)
    level = jax.random.uniform(level_key, (NZ, NY, NX), jnp.float32) * math.log(10.0)
    rising = 1.0 + 2.0 * jnp.arange(NZ, dtype=jnp.float32) / max(NZ - 1, 1)
    scales = jnp.exp(level) * rising[:, None, None] / 9.65 * float(NCELL * RANK) ** (-0.25)
    return (entries * scales[..., None]).astype(jnp.float32)


def draw_factor_obs(key, part):
    return factor_draw(key, 11)


def draw_factor_ctrl(key, part):
    return factor_draw(key, 23)


def block_levels(rng, dims, pieces, smallest, high):
    def one(dim, parts):
        heights = jax.random.uniform(jax.random.fold_in(jax.random.fold_in(rng, 6), dim), (parts,), jnp.float32, smallest / len(pieces), high / len(pieces))
        return jnp.repeat(jnp.exp(heights), dims[dim] // parts).reshape((-1,) + (1,) * (len(dims) - dim - 1))

    level = one(*pieces[0])
    for cut in pieces[1:]:
        level = level * one(*cut)
    return level


def centred(rng, shape, spread, limit, cuts=(), kind=jnp.bfloat16):
    values = spread * jax.random.normal(rng, shape, jnp.float32)
    if cuts:
        values = values * block_levels(rng, shape, cuts, -0.22, 0.18)
    return jnp.clip(values, -limit, limit).astype(kind)


def setup_inputs(seed: int = 0) -> dict:
    key_list = jax.random.split(jax.random.key(seed), 8)
    factor_obs = draw_factor_obs(jax.random.fold_in(key_list[7], 71), 0)
    factor_ctrl = draw_factor_ctrl(jax.random.fold_in(key_list[7], 71), 0)
    diffusivity = jnp.clip(jnp.exp(math.log(2.0) - 1.3862944 * jax.random.uniform(key_list[2], (NZ, NYX), jnp.float32) ** block_levels(key_list[2], (NZ, NYX), ((0, 32), (1, 4)), -0.2, 0.2)), 0.5, 2.0)
    input_map = centred(key_list[3], (NIN, NZ, NYX), (max(NCELL // RANK // 32, 1)) ** -0.5, 1.0, ((1, 32), (2, 4)), jnp.float32)
    output_map = centred(key_list[4], (NOUT, NZ, NYX), (max(NCELL // RANK // 32, 1)) ** -0.5, 1.0, ((1, 32), (2, 4)), jnp.float32)
    start_block = centred(key_list[5], (RANK, RMAX), 1.0, 6.0, (), jnp.float32)
    order = jax.random.randint(key_list[6], (1,), RMAX // 2, RMAX + 1).astype(jnp.int32)
    return dict(factor_obs=factor_obs, factor_ctrl=factor_ctrl, diffusivity=diffusivity, input_map=input_map, output_map=output_map, start_block=start_block, order=order)


def matmul(first, second):
    return jnp.dot(first.astype(jnp.float32), second.astype(jnp.float32), precision=lax.Precision.HIGHEST, preferred_element_type=jnp.float32)

def orthonormal(start):
    gram = matmul(start.T, start)
    lower_factor = jnp.linalg.cholesky(gram)
    return lax.linalg.triangular_solve(lower_factor, start, left_side=False, lower=True, transpose_a=True)

def subspace_bases(cross_gram, start_block):
    right_basis = orthonormal(matmul(cross_gram.T, start_block))
    left_basis = orthonormal(matmul(cross_gram, right_basis))
    for repeat in range(POWER - 1):
        right_basis = orthonormal(matmul(cross_gram.T, left_basis))
        left_basis = orthonormal(matmul(cross_gram, right_basis))
    return (left_basis, right_basis)

def apply_stencil(field, conduct):
    padded = jnp.pad(field, ((1, 1), (1, 1), (1, 1), (0, 0)))
    center = padded[1:-1, 1:-1, 1:-1]
    beside = padded[2:, 1:-1, 1:-1] + padded[:-2, 1:-1, 1:-1]
    beside = beside + padded[1:-1, 2:, 1:-1] + padded[1:-1, :-2, 1:-1]
    beside = beside + padded[1:-1, 1:-1, 2:] + padded[1:-1, 1:-1, :-2]
    return conduct[..., None] * (beside - 6.0 * center) / 6.0

def reference(factor_obs, factor_ctrl, diffusivity, input_map, output_map, start_block, order):
    cell_count = NZ * NY * NX
    observe = factor_obs.reshape(cell_count, RANK)
    control = factor_ctrl.reshape(cell_count, RANK)
    cross_gram = matmul(observe.T, control)
    left_basis, right_basis = subspace_bases(cross_gram, start_block)
    ctrl_space = matmul(control, right_basis)
    obs_space = matmul(observe, left_basis)
    conduct = diffusivity.reshape(NZ, NY, NX)
    applied = apply_stencil(ctrl_space.reshape(NZ, NY, NX, RMAX), conduct).reshape(cell_count, RMAX)
    kept_mask = (jnp.arange(RMAX, dtype=jnp.int32) < order[0]).astype(jnp.float32)
    square_mask = kept_mask[:, None] * kept_mask[None, :]
    reduced_mass = square_mask * matmul(left_basis.T, matmul(cross_gram, right_basis))
    reduced_state = square_mask * matmul(obs_space.T, applied)
    drive = input_map.reshape(NIN, cell_count)
    sense = output_map.reshape(NOUT, cell_count)
    reduced_input = kept_mask[:, None] * matmul(drive, obs_space).T
    reduced_output = kept_mask[None, :] * matmul(sense, ctrl_space)
    return (reduced_mass, reduced_state, reduced_input, reduced_output)
```

```python
import jax
import jax.numpy as jnp
from jax import lax
from jax.experimental import pallas as pl
from jax.experimental.pallas import tpu as pltpu
from jax.sharding import Mesh
from jax.sharding import PartitionSpec as P

SLAB = ("slab_0", "slab_1", "slab_2")

MESH = pl.DeviceIdType.MESH
STEP = 16
FLOOR = 2e-4


def position():
    z, y, c, x = (lax.axis_index(n) for n in ("slab_0", "slab_1", "slab_2", "sub"))
    return z, y, c, x


def peer_near(d):
    z, y, c, x = position()
    return (z, lax.rem(y + d * c, 4), c, lax.rem(x + d * (1 - c), 4))


def peer_next(d):
    z, y, c, x = position()
    return (z, lax.rem(y + d * (1 - c), 4), c, lax.rem(x + d * c, 4))


def peer_far(d):
    z, y, c, x = position()
    return (lax.rem(z + d, 4), y, c, x)


def partner():
    z, y, c, x = position()
    return (z, y, 1 - c, x)


def meet():
    barrier = pltpu.get_barrier_semaphore()
    pl.semaphore_signal(barrier, inc=1, device_id=partner(), device_id_type=MESH)
    for peers in (peer_near, peer_next, peer_far):
        for d in (1, 2, 3):
            pl.semaphore_signal(barrier, inc=1, device_id=peers(d), device_id_type=MESH)
    pl.semaphore_wait(barrier, 10)


def remote(src, dst, send, recv, to):
    return pltpu.make_async_remote_copy(
        src_ref=src, dst_ref=dst, send_sem=send, recv_sem=recv, device_id=to, device_id_type=MESH
    )


def rows(start, count):
    return pl.ds(pl.multiple_of(start, 8), count)


def big_kernel(x_ref, o_ref, in_c, acc_c, in_1, acc_1, in_2, acc_2, in_z, send, recv):
    z, y, c, x = position()
    near = x * (1 - c) + y * c
    nxt = y * (1 - c) + x * c
    half = x_ref.shape[0] // 2
    quarter = half // 4
    piece = quarter // 4
    meet()
    copy = remote(x_ref.at[rows((1 - c) * half, half)], in_c, send.at[0], recv.at[0], partner())
    copy.start()
    copy.wait()
    acc_c[...] = x_ref[rows(c * half, half), :] + in_c[...]
    copies = []
    for d in (1, 2, 3):
        copies.append(
            remote(
                acc_c.at[rows(lax.rem(near + d, 4) * quarter, quarter)],
                in_1.at[d - 1], send.at[d], recv.at[d], peer_near(d),
            )
        )
        copies[-1].start()
    for copy in copies:
        copy.wait()
    acc_1[...] = (acc_c[rows(near * quarter, quarter), :] + in_1[0]) + (in_1[1] + in_1[2])
    copies = []
    for d in (1, 2, 3):
        copies.append(
            remote(
                acc_1.at[rows(lax.rem(nxt + d, 4) * piece, piece)],
                in_2.at[d - 1], send.at[3 + d], recv.at[3 + d], peer_next(d),
            )
        )
        copies[-1].start()
    for copy in copies:
        copy.wait()
    mine = (acc_1[rows(nxt * piece, piece), :] + in_2[0]) + (in_2[1] + in_2[2])
    acc_2[...] = mine
    copies = []
    for d in (1, 2, 3):
        copies.append(
            remote(acc_2, in_z.at[z], send.at[6 + d], recv.at[6 + d], peer_far(d))
        )
        copies[-1].start()
    in_z[z] = mine
    for copy in copies:
        copy.wait()
    low = c * half + near * quarter
    at = low + nxt * piece
    o_ref[rows(at, piece), :] = (in_z[0] + in_z[1]) + (in_z[2] + in_z[3])
    copies = []
    for d in (1, 2, 3):
        block = o_ref.at[rows(at, piece)]
        copies.append(remote(block, block, send.at[9 + d], recv.at[9 + d], peer_next(d)))
        copies[-1].start()
    for copy in copies:
        copy.wait()
    copies = []
    for d in (1, 2, 3):
        block = o_ref.at[rows(low, quarter)]
        copies.append(remote(block, block, send.at[12 + d], recv.at[12 + d], peer_near(d)))
        copies[-1].start()
    for copy in copies:
        copy.wait()
    block = o_ref.at[rows(c * half, half)]
    copy = remote(block, block, send.at[16], recv.at[16], partner())
    copy.start()
    copy.wait()


def total_big(value):
    n, w = value.shape
    f = jnp.float32
    vm = pl.BlockSpec(memory_space=pltpu.VMEM)
    return pl.pallas_call(
        big_kernel,
        out_shape=jax.ShapeDtypeStruct(value.shape, f),
        in_specs=[vm],
        out_specs=vm,
        scratch_shapes=[
            pltpu.VMEM((n // 2, w), f),
            pltpu.VMEM((n // 2, w), f),
            pltpu.VMEM((3, n // 8, w), f),
            pltpu.VMEM((n // 8, w), f),
            pltpu.VMEM((3, n // 32, w), f),
            pltpu.VMEM((n // 32, w), f),
            pltpu.VMEM((4, n // 32, w), f),
            pltpu.SemaphoreType.DMA((17,)),
            pltpu.SemaphoreType.DMA((17,)),
        ],
        compiler_params=pltpu.CompilerParams(collective_id=0, has_side_effects=True),
        name="total_big",
    )(value)


def small_kernel(x_ref, o_ref, in_c, acc, in_1, in_2, in_3, send, recv):
    z, y, c, x = position()
    near = x * (1 - c) + y * c
    nxt = y * (1 - c) + x * c
    half = x_ref.shape[0] // 2
    meet()
    copy = remote(x_ref.at[rows((1 - c) * half, half)], in_c, send.at[0], recv.at[0], partner())
    copy.start()
    copy.wait()
    value = x_ref[rows(c * half, half), :] + in_c[...]
    stages = ((in_1, near, peer_near, 1), (in_2, nxt, peer_next, 4), (in_3, z, peer_far, 7))
    for stage, (into, me, peers, first) in enumerate(stages):
        acc[stage] = value
        copies = []
        for d in (1, 2, 3):
            k = first + d - 1
            copies.append(remote(acc.at[stage], into.at[me], send.at[k], recv.at[k], peers(d)))
            copies[-1].start()
        into[me] = value
        for copy in copies:
            copy.wait()
        value = (into[0] + into[1]) + (into[2] + into[3])
    block = o_ref.at[rows(c * half, half)]
    o_ref[rows(c * half, half), :] = value
    copy = remote(block, block, send.at[10], recv.at[10], partner())
    copy.start()
    copy.wait()


def total_small(value):
    n, w = value.shape
    f = jnp.float32
    vm = pl.BlockSpec(memory_space=pltpu.VMEM)
    return pl.pallas_call(
        small_kernel,
        out_shape=jax.ShapeDtypeStruct(value.shape, f),
        in_specs=[vm],
        out_specs=vm,
        scratch_shapes=[
            pltpu.VMEM((n // 2, w), f),
            pltpu.VMEM((3, n // 2, w), f),
            pltpu.VMEM((4, n // 2, w), f),
            pltpu.VMEM((4, n // 2, w), f),
            pltpu.VMEM((4, n // 2, w), f),
            pltpu.SemaphoreType.DMA((11,)),
            pltpu.SemaphoreType.DMA((11,)),
        ],
        compiler_params=pltpu.CompilerParams(collective_id=1, has_side_effects=True),
        name="total_small",
    )(value)


def split(value):
    high = value.astype(jnp.bfloat16)
    return high, (value - high.astype(jnp.float32)).astype(jnp.bfloat16)


def mul(first, second, contract):
    return lax.dot_general(
        first, second, (((contract[0],), (contract[1],)), ((), ())),
        preferred_element_type=jnp.float32,
    )


def gram_kernel(o_ref, c_ref, out_ref):
    @pl.when(pl.program_id(0) == 0)
    def _():
        out_ref[...] = jnp.zeros_like(out_ref)

    o_high, o_low = split(o_ref[...])
    c_high, c_low = split(c_ref[...])
    out_ref[...] += (
        mul(o_high, c_high, (0, 0)) + mul(o_high, c_low, (0, 0)) + mul(o_low, c_high, (0, 0))
    )


def gram(observe, control, block=1024):
    cells, rank = observe.shape
    spec = pl.BlockSpec((block, rank), lambda k: (k, 0))
    return pl.pallas_call(
        gram_kernel,
        grid=(cells // block,),
        out_shape=jax.ShapeDtypeStruct((rank, rank), jnp.float32),
        in_specs=[spec, spec],
        out_specs=pl.BlockSpec((rank, rank), lambda k: (0, 0)),
        compiler_params=pltpu.CompilerParams(dimension_semantics=("arbitrary",)),
        name="gram",
    )(observe, control)


def product(first, second, contract):
    return lax.dot_general(
        first, second, (((contract[0],), (contract[1],)), ((), ())),
        precision=lax.Precision.HIGHEST, preferred_element_type=jnp.float32,
    )


def factor(pairs):
    n = pairs[0][0].shape[0]
    f = jnp.float32
    row = lax.broadcasted_iota(jnp.int32, (STEP, n), 0)
    least = None
    eye = (
        lax.broadcasted_iota(jnp.int32, (n, n), 0) == lax.broadcasted_iota(jnp.int32, (n, n), 1)
    ).astype(f)
    for a, b in pairs:
        b[...] = eye
    for first in range(0, n, STEP):
        here = slice(first, first + STEP)
        work = []
        for a, b in pairs:
            across = a[here, :]
            cols = [
                jnp.broadcast_to(across[:, first + j : first + j + 1], (STEP, n))
                for j in range(STEP)
            ]
            work.append([across, b[here, :], cols, jnp.ones((STEP, n), f)])
        for j in range(STEP):
            for item in work:
                across, inverse, cols, pivots = item
                pivot = jnp.broadcast_to(cols[j][j : j + 1, :], (STEP, n))
                item[3] = jnp.where(row == j, pivot, pivots)
                if j == STEP - 1:
                    continue
                ratio = jnp.where(row > j, cols[j] / pivot, 0.0)
                for i in range(j + 1, STEP):
                    cols[i] = cols[i] - ratio * cols[i][j : j + 1, :]
                item[0] = across - ratio * across[j : j + 1, :]
                item[1] = inverse - ratio * inverse[j : j + 1, :]
        for (a, b), (across, inverse, cols, pivots) in zip(pairs, work):
            diag = jnp.sum(
                jnp.where(
                    lax.broadcasted_iota(jnp.int32, (STEP, n), 1) == row + first, a[here, :], 0.0
                ),
                axis=1,
                keepdims=True,
            )
            share = jnp.min(pivots[:, :1] / diag)
            least = share if least is None else jnp.minimum(least, share)
            scale = lax.rsqrt(pivots)
            upper = across * scale
            lower = inverse * scale
            a[here, :] = jnp.where(
                lax.broadcasted_iota(jnp.int32, (STEP, n), 1) >= row + first, upper, 0.0
            )
            b[here, :] = lower
            if first + STEP < n:
                rest = slice(first + STEP, n)
                change = product(upper, jnp.concatenate([upper, lower], axis=1), (0, 0))
                a[rest, :] = a[rest, :] - change[rest, :n]
                b[rest, :] = b[rest, :] - change[rest, n:]
    return least


def unit_rows(value):
    return value * lax.rsqrt(jnp.sum(value * value, axis=1, keepdims=True))


def bases_kernel(order_ref, m_ref, s_ref, right_ref, left_ref, mass_ref, a3, b3, a4, b4, y3, y4):
    n = a3.shape[0]
    m = m_ref
    y1 = unit_rows(product(s_ref[...].T, m[...], (1, 0)))
    y2 = unit_rows(product(y1, m[...], (1, 1)))
    y3[...] = unit_rows(product(y2, m[...], (1, 0)))
    y4[...] = product(y3[...], m[...], (1, 1))
    a3[...] = product(y3[...], y3[...], (1, 1))
    a4[...] = product(y4[...], y4[...], (1, 1))
    least = factor(((a3, b3), (a4, b4)))

    y3[...] = product(b3[...], y3[...], (1, 0))
    y4[...] = product(b4[...], y4[...], (1, 0))
    mass_ref[...] = product(a4[...], b3[...], (1, 1))

    @pl.when(jnp.logical_not(least > FLOOR))
    def _():
        y3[...] = s_ref[...].T

        def sweep(step, _):
            y4[...] = product(y3[...], m[...], (1, 0))
            a3[...] = product(y4[...], y4[...], (1, 1))
            factor(((a3, b3),))
            y3[...] = product(b3[...], y4[...], (1, 0))
            y4[...] = product(y3[...], m[...], (1, 1))
            a3[...] = product(y4[...], y4[...], (1, 1))
            a4[...] = y4[:, :n]
            factor(((a3, b3),))
            left_ref[...] = product(b3[...], y4[...], (1, 0))
            right_ref[...] = y3[...]
            mass_ref[...] = product(left_ref[...], y4[...], (1, 1))
            y3[...] = left_ref[...]
            return 0

        lax.fori_loop(0, 2, sweep, 0)
        y3[...] = right_ref[...]
        y4[...] = left_ref[...]

    order = order_ref[0]
    down = (lax.broadcasted_iota(jnp.int32, (n, n), 0) < order).astype(jnp.float32)
    along = (lax.broadcasted_iota(jnp.int32, (n, n), 1) < order).astype(jnp.float32)
    right_ref[...] = y3[...] * down[:, :1]
    left_ref[...] = y4[...] * down[:, :1]
    mass_ref[...] = mass_ref[...] * down * along


def bases(cross_gram, start_block, order):
    rank, n = start_block.shape
    f = jnp.float32
    vm = pl.BlockSpec(memory_space=pltpu.VMEM)
    return pl.pallas_call(
        bases_kernel,
        out_shape=(
            jax.ShapeDtypeStruct((n, rank), f),
            jax.ShapeDtypeStruct((n, rank), f),
            jax.ShapeDtypeStruct((n, n), f),
        ),
        in_specs=[pl.BlockSpec(memory_space=pltpu.SMEM), vm, vm],
        out_specs=(vm, vm, vm),
        scratch_shapes=[pltpu.VMEM((n, n), f)] * 4 + [pltpu.VMEM((n, rank), f)] * 2,
        name="bases",
    )(order, cross_gram, start_block)

def padded_2(value, sides, width):
    edges = {}
    for axis, dim in sides:
        count, length = (lax.axis_size(axis), value.shape[dim])
        up = [(i, (i + 1) % count) for i in range(count - 1)]
        last = lax.slice_in_dim(value, length - width, length, axis=dim)
        initial = lax.slice_in_dim(value, 0, width, axis=dim)
        edges[dim] = (
            lax.ppermute(last, axis, up),
            lax.ppermute(initial, axis, [(b, a) for a, b in up]),
        )
    done = []
    for _, dim in sides:
        low, high = edges[dim]
        around = [(width, width) if d in done else (0, 0) for d in range(value.ndim)]
        value = jnp.concatenate([jnp.pad(low, around), value, jnp.pad(high, around)], axis=dim)
        done.append(dim)
    return value


def matmul(first, second, contract):
    return lax.dot_general(
        first, second, (((contract[0],), (contract[1],)), ((), ())),
        precision=lax.Precision.HIGH, preferred_element_type=jnp.float32,
    )


def stencil_padded(padded, conduct):
    center = padded[1:-1, 1:-1]
    beside = padded[2:, 1:-1] + padded[:-2, 1:-1] + padded[1:-1, 2:] + padded[1:-1, :-2]
    along = jnp.pad(center, ((0, 0), (0, 0), (1, 1), (0, 0)))
    beside = beside + along[:, :, 2:] + along[:, :, :-2]
    return conduct[..., None] * (beside - 6.0 * center) / 6.0


def on_device(factor_obs, factor_ctrl, diffusivity, input_map, output_map, start_block, order):
    plane_count, line_count, point_count, rank_count = factor_ctrl.shape
    cell_count = plane_count * line_count * point_count
    observe = factor_obs.reshape(cell_count, rank_count)
    control = factor_ctrl.reshape(cell_count, rank_count)
    conduct = diffusivity.reshape(plane_count, line_count, point_count)
    drive = input_map.reshape(input_map.shape[0], cell_count)
    sense = output_map.reshape(output_map.shape[0], cell_count)
    basis_count = start_block.shape[1]
    cross_gram = total_big(gram(observe, control))
    right, left, reduced_mass = bases(cross_gram, start_block, order)
    ctrl_space = matmul(control, right, (1, 1))
    padded = padded_2(
        ctrl_space.reshape(plane_count, line_count, point_count, basis_count),
        ((SLAB, 0), ("sub", 1)),
        1,
    )
    obs_space = matmul(observe, left, (1, 1))
    applied = stencil_padded(padded, conduct).reshape(cell_count, basis_count)
    parts = jnp.concatenate(
        [
            matmul(obs_space, applied, (0, 0)),
            matmul(drive, obs_space, (1, 0)),
            matmul(sense, ctrl_space, (1, 0)),
            jnp.zeros((8, basis_count), jnp.float32),
        ]
    )
    whole = total_small(parts)
    n = basis_count
    return (reduced_mass, whole[:n], whole[n : n + 4].T, whole[n + 4 : n + 8])


def solution(mesh):
    torus = Mesh(
        mesh.devices.reshape(4, 4, 2, mesh.shape["sub"]), ("slab_0", "slab_1", "slab_2", "sub")
    )
    placed = (
        P(SLAB, "sub", None, None),
        P(SLAB, "sub", None, None),
        P(SLAB, "sub"),
        P(None, SLAB, "sub"),
        P(None, SLAB, "sub"),
        P(),
        P(),
    )
    return jax.shard_map(
        on_device, mesh=torus, in_specs=placed, out_specs=(P(), P(), P(), P()), check_vma=False
    )
```

```python
import jax
import jax.numpy as jnp
from jax import lax
from jax.experimental import pallas as pl
from jax.experimental.pallas import tpu as pltpu
from jax.sharding import Mesh
from jax.sharding import PartitionSpec as P

SLAB = ("slab_0", "slab_1", "slab_2")

MESH = pl.DeviceIdType.MESH
STEP = 16
FLOOR = 2e-4


def position():
    z, y, c, x = (lax.axis_index(n) for n in ("slab_0", "slab_1", "slab_2", "sub"))
    return z, y, c, x


def peer_near(d):
    z, y, c, x = position()
    return (z, lax.rem(y + d * c, 4), c, lax.rem(x + d * (1 - c), 4))


def peer_next(d):
    z, y, c, x = position()
    return (z, lax.rem(y + d * (1 - c), 4), c, lax.rem(x + d * c, 4))


def peer_far(d):
    z, y, c, x = position()
    return (lax.rem(z + d, 4), y, c, x)


def partner():
    z, y, c, x = position()
    return (z, y, 1 - c, x)


def meet():
    barrier = pltpu.get_barrier_semaphore()
    pl.semaphore_signal(barrier, inc=1, device_id=partner(), device_id_type=MESH)
    for peers in (peer_near, peer_next, peer_far):
        for d in (1, 2, 3):
            pl.semaphore_signal(barrier, inc=1, device_id=peers(d), device_id_type=MESH)
    pl.semaphore_wait(barrier, 10)


def remote(src, dst, send, recv, to):
    return pltpu.make_async_remote_copy(
        src_ref=src, dst_ref=dst, send_sem=send, recv_sem=recv, device_id=to, device_id_type=MESH
    )


def rows(start, count):
    return pl.ds(pl.multiple_of(start, 8), count)


def big_kernel(x_ref, o_ref, in_c, acc_c, in_1, acc_1, in_2, acc_2, in_z, send, recv):
    z, y, c, x = position()
    near = x * (1 - c) + y * c
    nxt = y * (1 - c) + x * c
    half = x_ref.shape[0] // 2
    quarter = half // 4
    piece = quarter // 4
    meet()
    copy = remote(x_ref.at[rows((1 - c) * half, half)], in_c, send.at[0], recv.at[0], partner())
    copy.start()
    copy.wait()
    acc_c[...] = x_ref[rows(c * half, half), :] + in_c[...]
    copies = []
    for d in (1, 2, 3):
        copies.append(
            remote(
                acc_c.at[rows(lax.rem(near + d, 4) * quarter, quarter)],
                in_1.at[d - 1], send.at[d], recv.at[d], peer_near(d),
            )
        )
        copies[-1].start()
    for copy in copies:
        copy.wait()
    acc_1[...] = (acc_c[rows(near * quarter, quarter), :] + in_1[0]) + (in_1[1] + in_1[2])
    copies = []
    for d in (1, 2, 3):
        copies.append(
            remote(
                acc_1.at[rows(lax.rem(nxt + d, 4) * piece, piece)],
                in_2.at[d - 1], send.at[3 + d], recv.at[3 + d], peer_next(d),
            )
        )
        copies[-1].start()
    for copy in copies:
        copy.wait()
    mine = (acc_1[rows(nxt * piece, piece), :] + in_2[0]) + (in_2[1] + in_2[2])
    acc_2[...] = mine
    copies = []
    for d in (1, 2, 3):
        copies.append(
            remote(acc_2, in_z.at[z], send.at[6 + d], recv.at[6 + d], peer_far(d))
        )
        copies[-1].start()
    in_z[z] = mine
    for copy in copies:
        copy.wait()
    low = c * half + near * quarter
    at = low + nxt * piece
    o_ref[rows(at, piece), :] = (in_z[0] + in_z[1]) + (in_z[2] + in_z[3])
    copies = []
    for d in (1, 2, 3):
        block = o_ref.at[rows(at, piece)]
        copies.append(remote(block, block, send.at[9 + d], recv.at[9 + d], peer_next(d)))
        copies[-1].start()
    for copy in copies:
        copy.wait()
    copies = []
    for d in (1, 2, 3):
        block = o_ref.at[rows(low, quarter)]
        copies.append(remote(block, block, send.at[12 + d], recv.at[12 + d], peer_near(d)))
        copies[-1].start()
    for copy in copies:
        copy.wait()
    block = o_ref.at[rows(c * half, half)]
    copy = remote(block, block, send.at[16], recv.at[16], partner())
    copy.start()
    copy.wait()


def total_big(value):
    n, w = value.shape
    f = jnp.float32
    vm = pl.BlockSpec(memory_space=pltpu.VMEM)
    return pl.pallas_call(
        big_kernel,
        out_shape=jax.ShapeDtypeStruct(value.shape, f),
        in_specs=[vm],
        out_specs=vm,
        scratch_shapes=[
            pltpu.VMEM((n // 2, w), f),
            pltpu.VMEM((n // 2, w), f),
            pltpu.VMEM((3, n // 8, w), f),
            pltpu.VMEM((n // 8, w), f),
            pltpu.VMEM((3, n // 32, w), f),
            pltpu.VMEM((n // 32, w), f),
            pltpu.VMEM((4, n // 32, w), f),
            pltpu.SemaphoreType.DMA((17,)),
            pltpu.SemaphoreType.DMA((17,)),
        ],
        compiler_params=pltpu.CompilerParams(collective_id=0, has_side_effects=True),
        name="total_big",
    )(value)


def split(value):
    high = value.astype(jnp.bfloat16)
    return high, (value - high.astype(jnp.float32)).astype(jnp.bfloat16)


def mul(first, second, contract):
    return lax.dot_general(
        first, second, (((contract[0],), (contract[1],)), ((), ())),
        preferred_element_type=jnp.float32,
    )


def gram_kernel(o_ref, c_ref, out_ref):
    @pl.when(pl.program_id(0) == 0)
    def _():
        out_ref[...] = jnp.zeros_like(out_ref)

    o_high, o_low = split(o_ref[...])
    c_high, c_low = split(c_ref[...])
    out_ref[...] += (
        mul(o_high, c_high, (0, 0)) + mul(o_high, c_low, (0, 0)) + mul(o_low, c_high, (0, 0))
    )


def gram(observe, control, block=1024):
    cells, rank = observe.shape
    spec = pl.BlockSpec((block, rank), lambda k: (k, 0))
    return pl.pallas_call(
        gram_kernel,
        grid=(cells // block,),
        out_shape=jax.ShapeDtypeStruct((rank, rank), jnp.float32),
        in_specs=[spec, spec],
        out_specs=pl.BlockSpec((rank, rank), lambda k: (0, 0)),
        compiler_params=pltpu.CompilerParams(dimension_semantics=("arbitrary",)),
        name="gram",
    )(observe, control)


def product(first, second, contract):
    return lax.dot_general(
        first, second, (((contract[0],), (contract[1],)), ((), ())),
        precision=lax.Precision.HIGHEST, preferred_element_type=jnp.float32,
    )


def factor(pairs):
    n = pairs[0][0].shape[0]
    f = jnp.float32
    row = lax.broadcasted_iota(jnp.int32, (STEP, n), 0)
    least = None
    eye = (
        lax.broadcasted_iota(jnp.int32, (n, n), 0) == lax.broadcasted_iota(jnp.int32, (n, n), 1)
    ).astype(f)
    for a, b in pairs:
        b[...] = eye
    for first in range(0, n, STEP):
        here = slice(first, first + STEP)
        work = []
        for a, b in pairs:
            across = a[here, :]
            cols = [
                jnp.broadcast_to(across[:, first + j : first + j + 1], (STEP, n))
                for j in range(STEP)
            ]
            work.append([across, b[here, :], cols, jnp.ones((STEP, n), f)])
        for j in range(STEP):
            for item in work:
                across, inverse, cols, pivots = item
                pivot = jnp.broadcast_to(cols[j][j : j + 1, :], (STEP, n))
                item[3] = jnp.where(row == j, pivot, pivots)
                if j == STEP - 1:
                    continue
                ratio = jnp.where(row > j, cols[j] / pivot, 0.0)
                for i in range(j + 1, STEP):
                    cols[i] = cols[i] - ratio * cols[i][j : j + 1, :]
                item[0] = across - ratio * across[j : j + 1, :]
                item[1] = inverse - ratio * inverse[j : j + 1, :]
        for (a, b), (across, inverse, cols, pivots) in zip(pairs, work):
            diag = jnp.sum(
                jnp.where(
                    lax.broadcasted_iota(jnp.int32, (STEP, n), 1) == row + first, a[here, :], 0.0
                ),
                axis=1,
                keepdims=True,
            )
            share = jnp.min(pivots[:, :1] / diag)
            least = share if least is None else jnp.minimum(least, share)
            scale = lax.rsqrt(pivots)
            upper = across * scale
            lower = inverse * scale
            a[here, :] = jnp.where(
                lax.broadcasted_iota(jnp.int32, (STEP, n), 1) >= row + first, upper, 0.0
            )
            b[here, :] = lower
            if first + STEP < n:
                rest = slice(first + STEP, n)
                change = product(upper, jnp.concatenate([upper, lower], axis=1), (0, 0))
                a[rest, :] = a[rest, :] - change[rest, :n]
                b[rest, :] = b[rest, :] - change[rest, n:]
    return least


def unit_rows(value):
    return value * lax.rsqrt(jnp.sum(value * value, axis=1, keepdims=True))


def bases_kernel(order_ref, m_ref, s_ref, right_ref, left_ref, mass_ref, a3, b3, a4, b4, y3, y4):
    n = a3.shape[0]
    m = m_ref
    y1 = unit_rows(product(s_ref[...].T, m[...], (1, 0)))
    y2 = unit_rows(product(y1, m[...], (1, 1)))
    y3[...] = unit_rows(product(y2, m[...], (1, 0)))
    y4[...] = product(y3[...], m[...], (1, 1))
    a3[...] = product(y3[...], y3[...], (1, 1))
    a4[...] = product(y4[...], y4[...], (1, 1))
    least = factor(((a3, b3), (a4, b4)))

    y3[...] = product(b3[...], y3[...], (1, 0))
    y4[...] = product(b4[...], y4[...], (1, 0))
    mass_ref[...] = product(a4[...], b3[...], (1, 1))

    @pl.when(jnp.logical_not(least > FLOOR))
    def _():
        y3[...] = s_ref[...].T

        def sweep(step, _):
            y4[...] = product(y3[...], m[...], (1, 0))
            a3[...] = product(y4[...], y4[...], (1, 1))
            factor(((a3, b3),))
            y3[...] = product(b3[...], y4[...], (1, 0))
            y4[...] = product(y3[...], m[...], (1, 1))
            a3[...] = product(y4[...], y4[...], (1, 1))
            a4[...] = y4[:, :n]
            factor(((a3, b3),))
            left_ref[...] = product(b3[...], y4[...], (1, 0))
            right_ref[...] = y3[...]
            mass_ref[...] = product(left_ref[...], y4[...], (1, 1))
            y3[...] = left_ref[...]
            return 0

        lax.fori_loop(0, 2, sweep, 0)
        y3[...] = right_ref[...]
        y4[...] = left_ref[...]

    order = order_ref[0]
    down = (lax.broadcasted_iota(jnp.int32, (n, n), 0) < order).astype(jnp.float32)
    along = (lax.broadcasted_iota(jnp.int32, (n, n), 1) < order).astype(jnp.float32)
    right_ref[...] = y3[...] * down[:, :1]
    left_ref[...] = y4[...] * down[:, :1]
    mass_ref[...] = mass_ref[...] * down * along


def bases(cross_gram, start_block, order):
    rank, n = start_block.shape
    f = jnp.float32
    vm = pl.BlockSpec(memory_space=pltpu.VMEM)
    return pl.pallas_call(
        bases_kernel,
        out_shape=(
            jax.ShapeDtypeStruct((n, rank), f),
            jax.ShapeDtypeStruct((n, rank), f),
            jax.ShapeDtypeStruct((n, n), f),
        ),
        in_specs=[pl.BlockSpec(memory_space=pltpu.SMEM), vm, vm],
        out_specs=(vm, vm, vm),
        scratch_shapes=[pltpu.VMEM((n, n), f)] * 4 + [pltpu.VMEM((n, rank), f)] * 2,
        name="bases",
    )(order, cross_gram, start_block)


def ring_peer(stage, d):
    z, y, c, x = position()
    k = lax.rem(stage + c, 3)
    on_x = (2 - k) * (1 - k) // 2
    on_y = k * (2 - k)
    on_z = k * (k - 1) // 2
    return (
        lax.rem(z + d * on_z, 4), lax.rem(y + d * on_y, 4), c, lax.rem(x + d * on_x, 4)
    )


def ring_place(stage):
    z, y, c, x = position()
    k = lax.rem(stage + c, 3)
    return x * ((2 - k) * (1 - k) // 2) + y * (k * (2 - k)) + z * (k * (k - 1) // 2)


def slab_peer(step):
    z, y, c, x = position()
    s = lax.rem((z * 4 + y) * 2 + c + step + 32, 32)
    return (s // 8, lax.rem(s // 2, 4), lax.rem(s, 2), x)


def sub_peer(step):
    z, y, c, x = position()
    return (z, y, c, lax.rem(x + step + 4, 4))


def shifted(value, step, length):
    rows_in = lax.broadcasted_iota(jnp.int32, value.shape, 0)
    at = lax.rem(rows_in, length)
    edge = 0 if step == 1 else length - 1
    return jnp.where(at == edge, 0.0, pltpu.roll(value, step % value.shape[0], 0))


def project_kernel(
    o_hbm, c_hbm, right_ref, left_ref, d_ref, drive_ref, sense_ref,
    state_ref, input_ref, output_ref,
    o_buf, c_buf, ctrl, obs, low_z, high_z, low_y, high_y, parts, in_c, acc, in_s,
    load, send, recv,
):
    planes, lines, points, width = ctrl.shape
    area = lines * points
    z, y, c, x = position()
    slab = (z * 4 + y) * 2 + c
    barrier = pltpu.get_barrier_semaphore()
    for to in (
        [partner(), slab_peer(2 * c - 1)]
        + [ring_peer(s, d) for s in range(3) for d in (1, 2, 3)]
    ):
        pl.semaphore_signal(barrier, inc=1, device_id=to, device_id_type=MESH)
    loads = {}
    order = (0, planes - 1) + tuple(range(1, planes - 1))
    for p in order:
        loads[p] = pltpu.make_async_copy(c_hbm.at[p], c_buf.at[p], load.at[p])
        loads[p].start()
    for p in range(planes):
        pltpu.make_async_copy(o_hbm.at[p], o_buf.at[p], load.at[planes + p]).start()
    r_high, r_low = split(right_ref[...])
    r_both = jnp.concatenate([r_high, r_low], axis=0)
    l_high, l_low = split(left_ref[...])
    l_both = jnp.concatenate([l_high, l_low], axis=0)

    down = remote(ctrl.at[0], high_z, send.at[0], recv.at[0], slab_peer(-1))
    up = remote(ctrl.at[planes - 1], low_z, send.at[1], recv.at[1], slab_peer(1))
    back = remote(ctrl.at[:, 0], high_y, send.at[2], recv.at[2], sub_peer(-1))
    ahead = remote(ctrl.at[:, lines - 1], low_y, send.at[3], recv.at[3], sub_peer(1))

    for p in order:
        loads[p].wait()
        high, low = split(c_buf[p].reshape(area, c_buf.shape[-1]))
        both = mul(high, r_both, (1, 1))
        value = both[:, :width] + both[:, width:] + mul(low, r_high, (1, 1))
        ctrl[p] = value.reshape(lines, points, width)
        if p == 0:
            pl.semaphore_wait(barrier, 11)

            @pl.when(slab > 0)
            def _():
                down.start()

        if p == planes - 1:
            @pl.when(slab < 31)
            def _():
                up.start()

    @pl.when(x > 0)
    def _():
        back.start()

    @pl.when(x < 3)
    def _():
        ahead.start()

    @pl.when(slab == 0)
    def _():
        low_z[...] = jnp.zeros_like(low_z)

    @pl.when(slab == 31)
    def _():
        high_z[...] = jnp.zeros_like(high_z)

    @pl.when(x == 0)
    def _():
        low_y[...] = jnp.zeros_like(low_y)

    @pl.when(x == 3)
    def _():
        high_y[...] = jnp.zeros_like(high_y)

    parts[...] = jnp.zeros_like(parts)

    def observe(p, _):
        pltpu.make_async_copy(o_hbm.at[p], o_buf.at[p], load.at[planes + p]).wait()
        high, low = split(o_buf[p].reshape(area, o_buf.shape[-1]))
        both = mul(l_both, high, (1, 1))
        value = both[:width] + both[width:] + mul(l_high, low, (1, 1))
        v_high, v_low = split(value)
        b_high, b_low = split(drive_ref[:, p, :])
        count = drive_ref.shape[0]
        parts[width : width + count, :] += (
            mul(b_high, v_high, (1, 1)) + mul(b_low, v_high, (1, 1)) + mul(b_high, v_low, (1, 1))
        )
        obs[p] = value * (d_ref[pl.ds(p, 1), :] / 6.0)
        return 0

    lax.fori_loop(0, planes, observe, 0)

    def spread(p):
        center = ctrl[p]
        below = low_z[...] if p == 0 else ctrl[p - 1]
        above = high_z[...] if p == planes - 1 else ctrl[p + 1]
        before = jnp.concatenate([low_y[p][None], ctrl[p, : lines - 1]], axis=0)
        after = jnp.concatenate([ctrl[p, 1:], high_y[p][None]], axis=0)
        flat = center.reshape(area, width)
        rest = (below + above + before + after).reshape(area, width)
        rest = rest + shifted(flat, 1, points) + shifted(flat, -1, points) - 6.0 * flat
        x_high, x_low = split(rest)
        f_high, f_low = split(flat)
        w_high = jnp.concatenate([x_high, f_high], axis=1)
        w_low = jnp.concatenate([x_low, f_low], axis=1)
        count = sense_ref.shape[0]
        ahead_rows = jnp.concatenate(
            [obs[p], sense_ref[:, p, :], jnp.zeros((8 - count, area), jnp.float32)], axis=0
        )
        a_high, a_low = split(ahead_rows)
        full = mul(a_high, w_high, (1, 0)) + mul(a_low, w_high, (1, 0)) + mul(a_high, w_low, (1, 0))
        parts[:width, :] += full[:width, :width]
        parts[width + 4 : width + 4 + count, :] += full[width : width + count, width:]

    @pl.when(x > 0)
    def _():
        back.wait_send()
        ahead.wait_recv()

    @pl.when(x < 3)
    def _():
        ahead.wait_send()
        back.wait_recv()

    for p in range(1, planes - 1):
        spread(p)

    @pl.when(slab > 0)
    def _():
        down.wait_send()
        up.wait_recv()

    @pl.when(slab < 31)
    def _():
        up.wait_send()
        down.wait_recv()

    spread(0)
    spread(planes - 1)

    half = parts.shape[0] // 2
    copy = remote(parts.at[rows((1 - c) * half, half)], in_c, send.at[4], recv.at[4], partner())
    copy.start()
    copy.wait()
    value = parts[rows(c * half, half), :] + in_c[...]
    for stage in range(3):
        me = ring_place(stage)
        acc[stage] = value
        copies = []
        for d in (1, 2, 3):
            k = 4 + 3 * stage + d
            copies.append(
                remote(
                    acc.at[stage], in_s.at[stage, me], send.at[k], recv.at[k], ring_peer(stage, d)
                )
            )
            copies[-1].start()
        in_s[stage, me] = value
        for copy in copies:
            copy.wait()
        value = (in_s[stage, 0] + in_s[stage, 1]) + (in_s[stage, 2] + in_s[stage, 3])
    acc[3] = value
    copy = remote(acc.at[3], in_s.at[3, c], send.at[14], recv.at[14], partner())
    copy.start()
    in_s[3, c] = value
    copy.wait()
    whole = jnp.concatenate([in_s[3, 0], in_s[3, 1]], axis=0)
    state_ref[...] = whole[:width]
    ends = whole[width : width + 8]
    input_ref[...] = ends.T[:, : input_ref.shape[1]]
    output_ref[...] = ends[4 : 4 + output_ref.shape[0]]


def project(observe, control, right, left, conduct, drive, sense):
    planes, lines, points, rank = control.shape
    n = right.shape[0]
    area = lines * points
    f = jnp.float32
    vm = pl.BlockSpec(memory_space=pltpu.VMEM)
    hbm = pl.BlockSpec(memory_space=pl.ANY)
    size = n + 16
    return pl.pallas_call(
        project_kernel,
        out_shape=(
            jax.ShapeDtypeStruct((n, n), f),
            jax.ShapeDtypeStruct((n, drive.shape[0]), f),
            jax.ShapeDtypeStruct((sense.shape[0], n), f),
        ),
        in_specs=[hbm, hbm, vm, vm, vm, vm, vm],
        out_specs=(vm, vm, vm),
        scratch_shapes=[
            pltpu.VMEM((planes, lines, points, rank), f),
            pltpu.VMEM((planes, lines, points, rank), f),
            pltpu.VMEM((planes, lines, points, n), f),
            pltpu.VMEM((planes, n, area), f),
            pltpu.VMEM((lines, points, n), f),
            pltpu.VMEM((lines, points, n), f),
            pltpu.VMEM((planes, points, n), f),
            pltpu.VMEM((planes, points, n), f),
            pltpu.VMEM((size, n), f),
            pltpu.VMEM((size // 2, n), f),
            pltpu.VMEM((4, size // 2, n), f),
            pltpu.VMEM((4, 4, size // 2, n), f),
            pltpu.SemaphoreType.DMA((2 * planes,)),
            pltpu.SemaphoreType.DMA((15,)),
            pltpu.SemaphoreType.DMA((15,)),
        ],
        compiler_params=pltpu.CompilerParams(
            collective_id=1, has_side_effects=True, vmem_limit_bytes=60 * 1024 * 1024
        ),
        name="project",
    )(observe, control, right, left, conduct, drive, sense)

def on_device(factor_obs, factor_ctrl, diffusivity, input_map, output_map, start_block, order):
    planes, lines, points, rank = factor_ctrl.shape
    cells = planes * lines * points
    cross_gram = total_big(
        gram(factor_obs.reshape(cells, rank), factor_ctrl.reshape(cells, rank))
    )
    right, left, reduced_mass = bases(cross_gram, start_block, order)
    state, inputs, outputs = project(
        factor_obs, factor_ctrl, right, left, diffusivity, input_map, output_map
    )
    return (reduced_mass, state, inputs, outputs)


def solution(mesh):
    torus = Mesh(
        mesh.devices.reshape(4, 4, 2, mesh.shape["sub"]), ("slab_0", "slab_1", "slab_2", "sub")
    )
    placed = (
        P(SLAB, "sub", None, None),
        P(SLAB, "sub", None, None),
        P(SLAB, "sub"),
        P(None, SLAB, "sub"),
        P(None, SLAB, "sub"),
        P(),
        P(),
    )
    return jax.shard_map(
        on_device, mesh=torus, in_specs=placed, out_specs=(P(), P(), P(), P()), check_vma=False
    )
```

```python
import jax
import jax.numpy as jnp
from jax import lax
from jax.experimental import pallas as pl
from jax.experimental.pallas import tpu as pltpu
from jax.sharding import Mesh
from jax.sharding import PartitionSpec as P

SLAB = ("slab_0", "slab_1", "slab_2")
STEP = 16
FLOOR = 1e-2

MESH = pl.DeviceIdType.MESH


def position():
    return tuple(lax.axis_index(n) for n in ("slab_0", "slab_1", "slab_2", "sub"))


def axis_of(stage):
    c = position()[2]
    k = lax.rem(stage + c, 3)
    return (2 - k) * (1 - k) // 2, k * (2 - k), k * (k - 1) // 2


def ring_peer(stage, d):
    z, y, c, x = position()
    on_x, on_y, on_z = axis_of(stage)
    return (
        lax.rem(z + d * on_z, 4), lax.rem(y + d * on_y, 4), c, lax.rem(x + d * on_x, 4)
    )


def ring_place(stage):
    z, y, c, x = position()
    on_x, on_y, on_z = axis_of(stage)
    return x * on_x + y * on_y + z * on_z


def partner():
    z, y, c, x = position()
    return (z, y, 1 - c, x)


def remote(src, dst, send, recv, to):
    return pltpu.make_async_remote_copy(
        src_ref=src, dst_ref=dst, send_sem=send, recv_sem=recv, device_id=to, device_id_type=MESH
    )


def rows(start, count):
    return pl.ds(pl.multiple_of(start, 8), count)


def split(value):
    high = value.astype(jnp.bfloat16)
    return high, (value - high.astype(jnp.float32)).astype(jnp.bfloat16)


def mul(first, second, contract):
    return lax.dot_general(
        first, second, (((contract[0],), (contract[1],)), ((), ())),
        preferred_element_type=jnp.float32,
    )


def cross_kernel(
    o_hbm, c_hbm, out_ref,
    o_buf, c_buf, c_high, c_low, turned, away, own, in_c, acc_c, in_1, acc_1, in_2, acc_2, in_3,
    load, send, recv,
):
    chunks = o_buf.shape[0]
    rank = c_buf.shape[-1]
    half = rank // 2
    quarter = half // 4
    piece = quarter // 4
    z, y, c, x = position()
    barrier = pltpu.get_barrier_semaphore()
    for to in [partner()] + [ring_peer(s, d) for s in range(3) for d in (1, 2, 3)]:
        pl.semaphore_signal(barrier, inc=1, device_id=to, device_id_type=MESH)
    loads = []
    for k in range(chunks):
        for j, (src, dst) in enumerate(((c_hbm, c_buf), (o_hbm, o_buf))):
            loads.append(pltpu.make_async_copy(src.at[k], dst.at[k], load.at[2 * k + j]))
            loads[-1].start()

    def columns(which):
        return pl.ds(pl.multiple_of(which * half, half), half)

    def thrice(both, high, low):
        full = mul(both, high, (1, 0))
        return full[:half] + full[half:] + mul(both[:half], low, (1, 0))

    def turn(value):
        high, low = split(value.T)
        return jnp.concatenate([high, low], axis=0)

    for k in range(chunks):
        loads[2 * k].wait()
        high, low = split(c_buf[k])
        c_high[k] = high
        c_low[k] = low
        loads[2 * k + 1].wait()
        term = thrice(turn(o_buf[k, :, columns(1 - c)]), high, low)
        away[...] = term if k == 0 else away[...] + term
    pl.semaphore_wait(barrier, 10)
    across = remote(away, in_c, send.at[0], recv.at[0], partner())
    across.start()

    first = ring_place(0)
    second = ring_place(1)
    third = ring_place(2)
    low_row = c * half + first * quarter
    at_row = low_row + second * piece

    def three(start, make):
        copies = []
        for d in (1, 2, 3):
            copies.append(make(d, send.at[start + d], recv.at[start + d]))
            copies[-1].start()
        return copies

    def done(copies):
        for copy in copies:
            copy.wait()

    def reduce_1(p):
        return three(3 * p, lambda d, s, r: remote(
            acc_c.at[p, rows(lax.rem(first + d, 4) * quarter, quarter)],
            in_1.at[p, d - 1], s, r, ring_peer(0, d)))

    def reduce_2(p):
        acc_1[p] = (acc_c[p, rows(first * quarter, quarter), :] + in_1[p, 0]) + (
            in_1[p, 1] + in_1[p, 2]
        )
        return three(6 + 3 * p, lambda d, s, r: remote(
            acc_1.at[p, rows(lax.rem(second + d, 4) * piece, piece)],
            in_2.at[p, d - 1], s, r, ring_peer(1, d)))

    def reduce_3(p):
        mine = (acc_1[p, rows(second * piece, piece), :] + in_2[p, 0]) + (in_2[p, 1] + in_2[p, 2])
        acc_2[p] = mine
        copies = three(12 + 3 * p, lambda d, s, r: remote(
            acc_2.at[p], in_3.at[p, third], s, r, ring_peer(2, d)))
        in_3[p, third] = mine
        return copies

    def gather_2(p):
        block = out_ref.at[rows(at_row, piece), p * half : (p + 1) * half]
        out_ref[rows(at_row, piece), p * half : (p + 1) * half] = (in_3[p, 0] + in_3[p, 1]) + (
            in_3[p, 2] + in_3[p, 3]
        )
        return three(18 + 3 * p, lambda d, s, r: remote(block, block, s, r, ring_peer(1, d)))

    def gather_1(p):
        block = out_ref.at[rows(low_row, quarter), p * half : (p + 1) * half]
        copies = three(24 + 3 * p, lambda d, s, r: remote(block, block, s, r, ring_peer(0, d)))
        copies.append(remote(block, block, send.at[31 + 4 * p], recv.at[31 + 4 * p], partner()))
        copies[-1].start()
        return copies

    def forward(p, copies):
        passed = [copies[3]]
        for d in (1, 2, 3):
            copies[d - 1].wait_recv()
            row = c * half + lax.rem(first + 4 - d, 4) * quarter
            block = out_ref.at[rows(row, quarter), p * half : (p + 1) * half]
            k = 31 + 4 * p + d
            passed.append(remote(block, block, send.at[k], recv.at[k], partner()))
            passed[-1].start()
        return passed

    for k in range(chunks):
        both = turn(o_buf[k, :, columns(c)])
        turned[k] = both
        term = thrice(both, c_high[k, :, :half], c_low[k, :, :half])
        own[...] = term if k == 0 else own[...] + term
    across.wait()
    acc_c[0] = own[...] + in_c[:, :half]
    moving_0 = reduce_1(0)
    for k in range(chunks):
        term = thrice(turned[k], c_high[k, :, half:], c_low[k, :, half:])
        own[...] = term if k == 0 else own[...] + term
    acc_c[1] = own[...] + in_c[:, half:]
    moving_1 = reduce_1(1)
    for stage in (reduce_2, reduce_3, gather_2, gather_1):
        done(moving_0)
        moving_0 = stage(0)
        done(moving_1)
        moving_1 = stage(1)
    passed_0 = forward(0, moving_0)
    passed_1 = forward(1, moving_1)
    for copies, passed in ((moving_0, passed_0), (moving_1, passed_1)):
        for copy in copies[:3]:
            copy.wait_send()
        done(passed)


def cross(observe, control, chunks=4):
    cells, rank = observe.shape
    f = jnp.float32
    b = jnp.bfloat16
    depth = cells // chunks
    half = rank // 2
    hbm = pl.BlockSpec(memory_space=pltpu.HBM)
    return pl.pallas_call(
        cross_kernel,
        out_shape=jax.ShapeDtypeStruct((rank, rank), f),
        in_specs=[hbm, hbm],
        out_specs=pl.BlockSpec(memory_space=pltpu.VMEM),
        scratch_shapes=[
            pltpu.VMEM((chunks, depth, rank), f),
            pltpu.VMEM((chunks, depth, rank), f),
            pltpu.VMEM((chunks, depth, rank), b),
            pltpu.VMEM((chunks, depth, rank), b),
            pltpu.VMEM((chunks, rank, depth), b),
            pltpu.VMEM((half, rank), f),
            pltpu.VMEM((half, half), f),
            pltpu.VMEM((half, rank), f),
            pltpu.VMEM((2, half, half), f),
            pltpu.VMEM((2, 3, half // 4, half), f),
            pltpu.VMEM((2, half // 4, half), f),
            pltpu.VMEM((2, 3, half // 16, half), f),
            pltpu.VMEM((2, half // 16, half), f),
            pltpu.VMEM((2, 4, half // 16, half), f),
            pltpu.SemaphoreType.DMA((2 * chunks,)),
            pltpu.SemaphoreType.DMA((39,)),
            pltpu.SemaphoreType.DMA((39,)),
        ],
        compiler_params=pltpu.CompilerParams(
            collective_id=0, has_side_effects=True, vmem_limit_bytes=50 * 1024 * 1024
        ),
        name="cross",
    )(observe.reshape(chunks, depth, rank), control.reshape(chunks, depth, rank))


def product(first, second, contract):
    return lax.dot_general(
        first, second, (((contract[0],), (contract[1],)), ((), ())),
        precision=lax.Precision.HIGHEST, preferred_element_type=jnp.float32,
    )


def narrow(first, second):
    f1 = first.astype(jnp.bfloat16).astype(jnp.float32)
    f2 = (first - f1).astype(jnp.bfloat16).astype(jnp.float32)
    f3 = first - f1 - f2
    s1 = second.astype(jnp.bfloat16).astype(jnp.float32)
    s2 = (second - s1).astype(jnp.bfloat16).astype(jnp.float32)
    s3 = second - s1 - s2
    a = jnp.concatenate([f1, f1, f2, f1, f2, f3], axis=0).T
    b = jnp.concatenate([s1, s2, s1, s3, s2, s1], axis=0)
    return lax.dot_general(
        a.astype(jnp.bfloat16), b.astype(jnp.bfloat16), (((1,), (0,)), ((), ())),
        preferred_element_type=jnp.float32,
    )


def factor(pairs):
    n = pairs[0][0].shape[0]
    f = jnp.float32
    row = lax.broadcasted_iota(jnp.int32, (STEP, n), 0)
    least = None
    eye = (
        lax.broadcasted_iota(jnp.int32, (n, n), 0) == lax.broadcasted_iota(jnp.int32, (n, n), 1)
    ).astype(f)
    for a, b in pairs:
        b[...] = eye
    for first in range(0, n, STEP):
        here = slice(first, first + STEP)
        work = []
        for a, b in pairs:
            across = a[here, :]
            cols = [
                jnp.broadcast_to(across[:, first + j : first + j + 1], (STEP, n))
                for j in range(STEP)
            ]
            work.append([across, b[here, :], cols, jnp.ones((STEP, n), f)])
        for j in range(STEP):
            for item in work:
                across, inverse, cols, pivots = item
                pivot = jnp.broadcast_to(cols[j][j : j + 1, :], (STEP, n))
                item[3] = jnp.where(row == j, pivot, pivots)
                if j == STEP - 1:
                    continue
                ratio = jnp.where(row > j, cols[j] / pivot, 0.0)
                for i in range(j + 1, STEP):
                    cols[i] = cols[i] - ratio * cols[i][j : j + 1, :]
                item[0] = across - ratio * across[j : j + 1, :]
                item[1] = inverse - ratio * inverse[j : j + 1, :]
        for (a, b), (across, inverse, cols, pivots) in zip(pairs, work):
            diag = jnp.sum(
                jnp.where(
                    lax.broadcasted_iota(jnp.int32, (STEP, n), 1) == row + first, a[here, :], 0.0
                ),
                axis=1,
                keepdims=True,
            )
            share = jnp.min(pivots[:, :1] / diag)
            least = share if least is None else jnp.minimum(least, share)
            scale = lax.rsqrt(pivots)
            upper = across * scale
            lower = inverse * scale
            a[here, :] = jnp.where(
                lax.broadcasted_iota(jnp.int32, (STEP, n), 1) >= row + first, upper, 0.0
            )
            b[here, :] = lower
            if first + STEP < n:
                rest = slice(first + STEP, n)
                change = narrow(upper, jnp.concatenate([upper, lower], axis=1))
                a[rest, :] = a[rest, :] - change[rest, :n]
                b[rest, :] = b[rest, :] - change[rest, n:]
    return least


def by_halves(first, high, low, contract):
    n = first.shape[0]
    f_high, f_low = split(first)
    both = mul(jnp.concatenate([f_high, f_low], axis=0), high, contract)
    return both[:n] + both[n:] + mul(f_high, low, contract)


def unit_rows(value):
    return value * lax.rsqrt(jnp.sum(value * value, axis=1, keepdims=True))


def bases_kernel(order_ref, m_ref, s_ref, right_ref, left_ref, mass_ref, a3, b3, a4, b4, y3, y4, high, low):
    n = a3.shape[0]
    m = m_ref
    high[...], low[...] = split(m[...])
    y1 = unit_rows(by_halves(s_ref[...].T, high[...], low[...], (1, 0)))
    y2 = unit_rows(by_halves(y1, high[...], low[...], (1, 1)))
    y3[...] = unit_rows(by_halves(y2, high[...], low[...], (1, 0)))
    y4[...] = by_halves(y3[...], high[...], low[...], (1, 1))
    a3[...] = product(y3[...], y3[...], (1, 1))
    a4[...] = product(y4[...], y4[...], (1, 1))
    least = factor(((a3, b3), (a4, b4)))

    y3[...] = product(b3[...], y3[...], (1, 0))
    y4[...] = product(b4[...], y4[...], (1, 0))
    mass_ref[...] = product(a4[...], b3[...], (1, 1))

    @pl.when(jnp.logical_not(least > FLOOR))
    def _():
        y3[...] = s_ref[...].T

        def sweep(step, _):
            y4[...] = product(y3[...], m[...], (1, 0))
            a3[...] = product(y4[...], y4[...], (1, 1))
            factor(((a3, b3),))
            y3[...] = product(b3[...], y4[...], (1, 0))
            y4[...] = product(y3[...], m[...], (1, 1))
            a3[...] = product(y4[...], y4[...], (1, 1))
            a4[...] = y4[:, :n]
            factor(((a3, b3),))
            left_ref[...] = product(b3[...], y4[...], (1, 0))
            right_ref[...] = y3[...]
            mass_ref[...] = product(left_ref[...], y4[...], (1, 1))
            y3[...] = left_ref[...]
            return 0

        lax.fori_loop(0, 2, sweep, 0)
        y3[...] = right_ref[...]
        y4[...] = left_ref[...]

    order = order_ref[0]
    down = (lax.broadcasted_iota(jnp.int32, (n, n), 0) < order).astype(jnp.float32)
    along = (lax.broadcasted_iota(jnp.int32, (n, n), 1) < order).astype(jnp.float32)
    right_ref[...] = y3[...] * down[:, :1]
    left_ref[...] = y4[...] * down[:, :1]
    mass_ref[...] = mass_ref[...] * down * along


def bases(cross_gram, start_block, order):
    rank, n = start_block.shape
    f = jnp.float32
    vm = pl.BlockSpec(memory_space=pltpu.VMEM)
    return pl.pallas_call(
        bases_kernel,
        out_shape=(
            jax.ShapeDtypeStruct((n, rank), f),
            jax.ShapeDtypeStruct((n, rank), f),
            jax.ShapeDtypeStruct((n, n), f),
        ),
        in_specs=[pl.BlockSpec(memory_space=pltpu.SMEM), vm, vm],
        out_specs=(vm, vm, vm),
        scratch_shapes=[pltpu.VMEM((n, n), f)] * 4 + [pltpu.VMEM((n, rank), f)] * 2
        + [pltpu.VMEM((rank, rank), jnp.bfloat16)] * 2,
        compiler_params=pltpu.CompilerParams(vmem_limit_bytes=16 * 1024 * 1024),
        cost_estimate=pl.CostEstimate(
            flops=8 * 6 * 2 * n * rank * rank, bytes_accessed=4 * rank * rank, transcendentals=0
        ),
        name="bases",
    )(order, cross_gram, start_block)


def slab_peer(step):
    z, y, c, x = position()
    s = lax.rem((z * 4 + y) * 2 + c + step + 32, 32)
    return (s // 8, lax.rem(s // 2, 4), lax.rem(s, 2), x)


def sub_peer(step):
    z, y, c, x = position()
    return (z, y, c, lax.rem(x + step + 4, 4))


def shifted(value, step, length):
    rows_in = lax.broadcasted_iota(jnp.int32, value.shape, 0)
    at = lax.rem(rows_in, length)
    edge = 0 if step == 1 else length - 1
    return jnp.where(at == edge, 0.0, pltpu.roll(value, step % value.shape[0], 0))


def project_kernel(
    c_ref, o_hbm, right_ref, left_ref, d_ref, drive_ref, sense_ref,
    out_ref,
    o_buf, ctrl, obs, low_z, high_z, low_y, high_y, parts, in_c, acc, in_s,
    load, send, recv,
):
    planes, lines, points, width = ctrl.shape
    area = lines * points
    z, y, c, x = position()
    slab = (z * 4 + y) * 2 + c
    barrier = pltpu.get_barrier_semaphore()
    for to in (
        [partner(), slab_peer(2 * c - 1)]
        + [ring_peer(s, d) for s in range(3) for d in (1, 2, 3)]
    ):
        pl.semaphore_signal(barrier, inc=1, device_id=to, device_id_type=MESH)
    order = (0, planes - 1) + tuple(range(1, planes - 1))
    for p in range(planes):
        pltpu.make_async_copy(o_hbm.at[p], o_buf.at[p], load.at[p]).start()
    r_high, r_low = split(right_ref[...])
    r_both = jnp.concatenate([r_high, r_low], axis=0)
    l_high, l_low = split(left_ref[...])
    l_both = jnp.concatenate([l_high, l_low], axis=0)

    down = remote(ctrl.at[0], high_z, send.at[0], recv.at[0], slab_peer(-1))
    up = remote(ctrl.at[planes - 1], low_z, send.at[1], recv.at[1], slab_peer(1))
    back = remote(ctrl.at[:, 0], high_y, send.at[2], recv.at[2], sub_peer(-1))
    ahead = remote(ctrl.at[:, lines - 1], low_y, send.at[3], recv.at[3], sub_peer(1))

    for p in order:
        high, low = split(c_ref[p].reshape(area, c_ref.shape[-1]))
        both = mul(high, r_both, (1, 1))
        value = both[:, :width] + both[:, width:] + mul(low, r_high, (1, 1))
        ctrl[p] = value.reshape(lines, points, width)
        if p == 0:
            pl.semaphore_wait(barrier, 11)

            @pl.when(slab > 0)
            def _():
                down.start()

        if p == planes - 1:
            @pl.when(slab < 31)
            def _():
                up.start()

    @pl.when(x > 0)
    def _():
        back.start()

    @pl.when(x < 3)
    def _():
        ahead.start()

    @pl.when(slab == 0)
    def _():
        low_z[...] = jnp.zeros_like(low_z)

    @pl.when(slab == 31)
    def _():
        high_z[...] = jnp.zeros_like(high_z)

    @pl.when(x == 0)
    def _():
        low_y[...] = jnp.zeros_like(low_y)

    @pl.when(x == 3)
    def _():
        high_y[...] = jnp.zeros_like(high_y)

    parts[...] = jnp.zeros_like(parts)

    def observe(p, _):
        pltpu.make_async_copy(o_hbm.at[p], o_buf.at[p], load.at[p]).wait()
        high, low = split(o_buf[p].reshape(area, o_buf.shape[-1]))
        both = mul(l_both, high, (1, 1))
        value = both[:width] + both[width:] + mul(l_high, low, (1, 1))
        v_high, v_low = split(value)
        b_high, b_low = split(drive_ref[:, p, :])
        count = drive_ref.shape[0]
        parts[width : width + count, :] += (
            mul(b_high, v_high, (1, 1)) + mul(b_low, v_high, (1, 1)) + mul(b_high, v_low, (1, 1))
        )
        obs[p] = value * (d_ref[pl.ds(p, 1), :] / 6.0)
        return 0

    lax.fori_loop(0, planes, observe, 0)

    def spread(p):
        center = ctrl[p]
        below = low_z[...] if p == 0 else ctrl[p - 1]
        above = high_z[...] if p == planes - 1 else ctrl[p + 1]
        before = jnp.concatenate([low_y[p][None], ctrl[p, : lines - 1]], axis=0)
        after = jnp.concatenate([ctrl[p, 1:], high_y[p][None]], axis=0)
        flat = center.reshape(area, width)
        rest = (below + above + before + after).reshape(area, width)
        rest = rest + shifted(flat, 1, points) + shifted(flat, -1, points) - 6.0 * flat
        x_high, x_low = split(rest)
        f_high, f_low = split(flat)
        w_high = jnp.concatenate([x_high, f_high], axis=1)
        w_low = jnp.concatenate([x_low, f_low], axis=1)
        count = sense_ref.shape[0]
        ahead_rows = jnp.concatenate(
            [obs[p], sense_ref[:, p, :], jnp.zeros((8 - count, area), jnp.float32)], axis=0
        )
        a_high, a_low = split(ahead_rows)
        full = mul(a_high, w_high, (1, 0)) + mul(a_low, w_high, (1, 0)) + mul(a_high, w_low, (1, 0))
        parts[:width, :] += full[:width, :width]
        parts[width + 4 : width + 4 + count, :] += full[width : width + count, width:]

    @pl.when(x > 0)
    def _():
        back.wait_send()
        ahead.wait_recv()

    @pl.when(x < 3)
    def _():
        ahead.wait_send()
        back.wait_recv()

    for p in range(1, planes - 1):
        spread(p)

    @pl.when(slab > 0)
    def _():
        down.wait_send()
        up.wait_recv()

    @pl.when(slab < 31)
    def _():
        up.wait_send()
        down.wait_recv()

    spread(0)
    spread(planes - 1)

    half = parts.shape[0] // 2
    copy = remote(parts.at[rows((1 - c) * half, half)], in_c, send.at[4], recv.at[4], partner())
    copy.start()
    copy.wait()
    value = parts[rows(c * half, half), :] + in_c[...]
    for stage in range(3):
        me = ring_place(stage)
        acc[stage] = value
        copies = []
        for d in (1, 2, 3):
            k = 4 + 3 * stage + d
            copies.append(
                remote(
                    acc.at[stage], in_s.at[stage, me], send.at[k], recv.at[k], ring_peer(stage, d)
                )
            )
            copies[-1].start()
        in_s[stage, me] = value
        for copy in copies:
            copy.wait()
        value = (in_s[stage, 0] + in_s[stage, 1]) + (in_s[stage, 2] + in_s[stage, 3])
    acc[3] = value
    copy = remote(acc.at[3], in_s.at[3, c], send.at[14], recv.at[14], partner())
    copy.start()
    in_s[3, c] = value
    copy.wait()
    out_ref[:half, :] = in_s[3, 0]
    out_ref[half:, :] = in_s[3, 1]


def finish_kernel(whole_ref, state_ref, input_ref, output_ref):
    n = state_ref.shape[0]
    count = input_ref.shape[0]
    state_ref[...] = whole_ref[:n, :]
    input_ref[...] = whole_ref[n : n + count, :]
    output_ref[...] = whole_ref[n + 4 : n + 4 + output_ref.shape[0], :]


def project(observe, control, right, left, conduct, drive, sense):
    planes, lines, points, rank = control.shape
    n = right.shape[0]
    area = lines * points
    f = jnp.float32
    vm = pl.BlockSpec(memory_space=pltpu.VMEM)
    hbm = pl.BlockSpec(memory_space=pltpu.HBM)
    size = n + 16
    whole = pl.pallas_call(
        project_kernel,
        out_shape=jax.ShapeDtypeStruct((size, n), f),
        in_specs=[vm, hbm] + [vm] * 5,
        out_specs=vm,
        scratch_shapes=[
            pltpu.VMEM((planes, lines, points, rank), f),
            pltpu.VMEM((planes, lines, points, n), f),
            pltpu.VMEM((planes, n, area), f),
            pltpu.VMEM((lines, points, n), f),
            pltpu.VMEM((lines, points, n), f),
            pltpu.VMEM((planes, points, n), f),
            pltpu.VMEM((planes, points, n), f),
            pltpu.VMEM((size, n), f),
            pltpu.VMEM((size // 2, n), f),
            pltpu.VMEM((4, size // 2, n), f),
            pltpu.VMEM((4, 4, size // 2, n), f),
            pltpu.SemaphoreType.DMA((planes,)),
            pltpu.SemaphoreType.DMA((15,)),
            pltpu.SemaphoreType.DMA((15,)),
        ],
        compiler_params=pltpu.CompilerParams(
            collective_id=1, has_side_effects=True, vmem_limit_bytes=42 * 1024 * 1024
        ),
        name="project",
    )(control, observe, right, left, conduct, drive, sense)
    state, inputs, outputs = pl.pallas_call(
        finish_kernel,
        out_shape=(
            jax.ShapeDtypeStruct((n, n), f),
            jax.ShapeDtypeStruct((drive.shape[0], n), f),
            jax.ShapeDtypeStruct((sense.shape[0], n), f),
        ),
        in_specs=[vm],
        out_specs=(vm, vm, vm),
        compiler_params=pltpu.CompilerParams(vmem_limit_bytes=4 * 1024 * 1024),
        name="finish",
    )(whole)
    return state, inputs.T, outputs

def on_device(factor_obs, factor_ctrl, diffusivity, input_map, output_map, start_block, order):
    planes, lines, points, rank = factor_ctrl.shape
    cells = planes * lines * points
    cross_gram = cross(factor_obs.reshape(cells, rank), factor_ctrl.reshape(cells, rank))
    right, left, reduced_mass = bases(cross_gram, start_block, order)
    state, inputs, outputs = project(
        factor_obs, factor_ctrl, right, left, diffusivity, input_map, output_map
    )
    return (reduced_mass, state, inputs, outputs)


def solution(mesh):
    torus = Mesh(
        mesh.devices.reshape(4, 4, 2, mesh.shape["sub"]), ("slab_0", "slab_1", "slab_2", "sub")
    )
    placed = (
        P(SLAB, "sub", None, None),
        P(SLAB, "sub", None, None),
        P(SLAB, "sub"),
        P(None, SLAB, "sub"),
        P(None, SLAB, "sub"),
        P(),
        P(),
    )
    return jax.shard_map(
        on_device, mesh=torus, in_specs=placed, out_specs=(P(), P(), P(), P()), check_vma=False
    )
```
